32 devices in a mesh: gx: 16 (over z, y, x), gy: 2 (over core).
Axes of the slice: x: 2, y: 2, z: 4, core: 2. Of those that a mesh axis runs over, the one named last changes fastest.
Arguments:
- droplets: float32 [2, 32, 32, 1024], P(None, None, 'gx', 'gy'), as said below
- moves: int32 [2, 32, 32, 1024], P(None, None, 'gx', 'gy'), may hold values from 0 to 8, as said below
- pairing: int32 [2, 32, 32, 1024], P(None, None, 'gx', 'gy'), may hold values from 0 to 31, as said below
- collisions: int32 [2, 16, 32, 1024], P(None, None, 'gx', 'gy'), may hold values from 0 to 3
Outputs:
- droplets_out: float32 [2, 32, 32, 1024], P(None, None, 'gx', 'gy')
- moments: float32 [2, 2, 16], replicated
The draws below stay inside these ranges and needn't reach their ends.
Inputs may be any that keep to these rules, and one draw needn't show every extreme that they name: `droplets`: entry 0 holds whole-number multiplicities from 24 to below 300, entry 1 masses from 0.05 to 2. `moves`: A code c means a step of c // 3 - 1 along x and c % 3 - 1 along y. In each step, slot and level, all droplets of one y-row take the same x-step and all droplets landing in one x-column take the same y-step, so every cell and slot receives exactly one droplet. `pairing`: for each step and cell, the entries along the slot dimension are a permutation of 0 to 31.
All inputs are finite; a program needn't handle non-finite values.
Results may differ from the reference program's by a relative error of at most 0.0003.
Values sent between devices are 32-bit elements; how exact they have to be, the bound alone decides.
A program may use at most 64 MiB of HBM per device.

```python
import jax
import jax.numpy as jnp
from jax import lax

SLOTS = 32
PAIRS = 16
STEPS = 2
LEVELS = 16
NX = 32
NY = 64


def draw_droplets(key, part):
    keys = jax.random.split(jax.random.fold_in(key, 303), 2)
    shape = (SLOTS, NX, NY, LEVELS)
    raw = jax.random.randint(keys[0], shape, 24, 96)
    x_index = lax.broadcasted_iota(jnp.int32, shape, 1)
    counts = (raw * (NX + 2 * x_index) // NX).astype(jnp.float32)
    uniform = jax.random.uniform(keys[1], shape, jnp.float32)
    masses = jnp.exp(jnp.log(0.05) + uniform * (jnp.log(2.0) - jnp.log(0.05)))
    return jnp.stack([counts, masses.astype(jnp.float32)]).reshape(2, SLOTS, NX, NY * LEVELS)


def draw_moves(key, part):
    table = jnp.array([-1, -1, 0, 1, 1], jnp.int32)
    row_key, col_key = jax.random.split(jax.random.fold_in(key, 101))
    shape = (STEPS, SLOTS, NX, NY, LEVELS)
    row_pick = table[jax.random.randint(row_key, (STEPS, SLOTS, 1, NY, LEVELS), 0, 5)]
    col_pick = table[jax.random.randint(col_key, (STEPS, SLOTS, NX, 1, LEVELS), 0, 5)]
    x_index = lax.broadcasted_iota(jnp.int32, shape, 2)
    landing = (x_index + row_pick) % NX
    step_y = jnp.take_along_axis(jnp.broadcast_to(col_pick, shape), landing, axis=2)
    codes = 3 * (row_pick + 1) + step_y + 1
    return codes.reshape(STEPS, SLOTS, NX, NY * LEVELS).astype(jnp.int32)


def draw_pairing(key, part):
    shape = (STEPS, SLOTS, NX, NY * LEVELS)
    scores = jax.random.randint(jax.random.fold_in(key, 202), shape, 0, 1048576) * SLOTS
    scores = scores + lax.broadcasted_iota(jnp.int32, shape, 1)
    return jnp.argsort(scores, axis=1, stable=True).astype(jnp.int32)


def touch_ends(drawn, own_key, least, top_value):
    longest = drawn.shape.index(max(drawn.shape))
    spots = []
    for shift in (0, 1):
        where = [jax.random.randint(jax.random.fold_in(own_key, axis), (), 0, length) for axis, length in enumerate(drawn.shape)]
        where[longest] = (where[longest] + shift) % drawn.shape[longest]
        spots.append(tuple(where))
    return drawn.at[spots[0]].set(least).at[spots[1]].set(top_value)


def setup_inputs(seed: int = 0) -> dict:
    streams_of = jax.random.split(jax.random.key(seed), 5)
    return {
        "droplets": draw_droplets(jax.random.fold_in(streams_of[4], 71), 0),
        "moves": draw_moves(jax.random.fold_in(streams_of[4], 71), 0),
        "pairing": draw_pairing(jax.random.fold_in(streams_of[4], 71), 0),
        "collisions": touch_ends(jax.random.randint(streams_of[3], (STEPS, PAIRS, NX, NY * LEVELS), 0, 4), jax.random.fold_in(streams_of[3], 1), 0, 3).astype(jnp.int32),
    }


count_unit = 4096.0


def migrate(state, codes):
    moved = jnp.zeros_like(state)
    for direction in range(9):
        step_x = direction // 3 - 1
        step_y = direction % 3 - 1
        chosen = jnp.where((codes == direction)[None], state, jnp.zeros_like(state))
        moved = moved + jnp.roll(chosen, (step_x, step_y), axis=(2, 3))
    return moved


def collide(first_count, second_count, first_mass, second_mass, tries):
    big_first = first_count >= second_count
    larger = jnp.where(big_first, first_count, second_count)
    smaller = jnp.where(big_first, second_count, first_count)
    larger_mass = jnp.where(big_first, first_mass, second_mass)
    smaller_mass = jnp.where(big_first, second_mass, first_mass)
    taken = jnp.minimum(tries, larger // smaller)
    remain = larger - taken * smaller
    splits = remain == 0
    halved = smaller // 2
    larger_new = jnp.where(splits, halved, remain)
    smaller_new = jnp.where(splits, smaller - halved, smaller)
    grown = smaller_mass + taken.astype(first_mass.dtype) * larger_mass
    larger_mass_new = jnp.where(splits, grown, larger_mass)
    first_new = jnp.where(big_first, larger_new, smaller_new)
    second_new = jnp.where(big_first, smaller_new, larger_new)
    first_mass_new = jnp.where(big_first, larger_mass_new, grown)
    second_mass_new = jnp.where(big_first, grown, larger_mass_new)
    return first_new, second_new, first_mass_new, second_mass_new


def coalesce(state, order, tries):
    counts = state[0].astype(jnp.int32)
    masses = state[1]
    counts_p = jnp.take_along_axis(counts, order, axis=0)
    masses_p = jnp.take_along_axis(masses, order, axis=0)
    first_new, second_new, first_mass, second_mass = collide(counts_p[0::2], counts_p[1::2], masses_p[0::2], masses_p[1::2], tries)
    counts_pair = jnp.stack([first_new, second_new], axis=1).reshape(counts_p.shape)
    masses_pair = jnp.stack([first_mass, second_mass], axis=1).reshape(masses_p.shape)
    inverse = jnp.argsort(order, axis=0).astype(jnp.int32)
    counts_new = jnp.take_along_axis(counts_pair, inverse, axis=0)
    masses_new = jnp.take_along_axis(masses_pair, inverse, axis=0)
    return jnp.stack([counts_new.astype(state.dtype), masses_new])


def level_moments(state):
    count_sum = jnp.sum(state[0], axis=(0, 1, 2))
    liquid_sum = jnp.sum(state[0] * state[1], axis=(0, 1, 2))
    return jnp.stack([count_sum, liquid_sum]) / (NX * NY * count_unit)


def reference(droplets, moves, pairing, collisions):
    state = droplets.reshape(2, SLOTS, NX, NY, LEVELS)
    codes = moves.reshape(STEPS, SLOTS, NX, NY, LEVELS)
    orders = pairing.reshape(STEPS, SLOTS, NX, NY, LEVELS)
    tries = collisions.reshape(STEPS, PAIRS, NX, NY, LEVELS)
    results = []
    for step in range(STEPS):
        state = migrate(state, codes[step])
        state = coalesce(state, orders[step], tries[step])
        results.append(level_moments(state))
    return state.reshape(droplets.shape), jnp.stack(results)
```

```python
import functools

import jax
import jax.numpy as jnp
from jax import lax
from jax.experimental import pallas as pl
from jax.experimental.pallas import tpu as pltpu
from jax.sharding import PartitionSpec as P

LEVELS = 16
LANES = 128
ROWS = 8
CHUNKS = 4
count_unit = 4096.0
MESH = pl.DeviceIdType.MESH


def roll(value, shift, axis):
    shift = shift % value.shape[axis]
    return value if shift == 0 else pltpu.roll(value, shift, axis)


def tree(values, bits):
    level = 0
    while len(values) > 1:
        values = [
            jnp.where(bits[level], values[i + 1], values[i]) for i in range(0, len(values), 2)
        ]
        level += 1
    return values[0]


def collide(na, nb, ma, mb, tries):
    first = na >= nb
    big, small = jnp.maximum(na, nb), jnp.minimum(na, nb)
    big_m, small_m = jnp.where(first, ma, mb), jnp.where(first, mb, ma)
    most = jnp.where(3.0 * small <= big, 3.0, jnp.where(2.0 * small <= big, 2.0, 1.0))
    taken = jnp.minimum(tries.astype(jnp.float32), most)
    remain = big - taken * small
    split = remain == 0.0
    half = jnp.floor(small * 0.5)
    big_new = jnp.where(split, half, remain)
    small_new = jnp.where(split, small - half, small)
    grown = small_m + taken * big_m
    big_m_new = jnp.where(split, grown, big_m)
    return (
        jnp.where(first, big_new, small_new),
        jnp.where(first, small_new, big_new),
        jnp.where(first, big_m_new, grown),
        jnp.where(first, grown, big_m_new),
    )


def kernel(
    nx, ny, slots, steps, scale,
    drops_hbm, moves_hbm, order_hbm, tries_hbm, out_hbm, mom_ref,
    cur, moves, order, tries, moved, paired, cy_ref,
    send_l, send_r, halo_l, halo_r,
    code_send, code_l, code_r,
    edge_send, edge_dn, edge_up,
    part_y, got_y, part_x, got_x,
    in_sem, out_sem, xs_sem, xl_sem, xr_sem, cs_sem, cl_sem, cr_sem,
    es_sem, ed_sem, eu_sem, ys_sem, yr_sem, gs_sem, gr_sem,
):
    gx, gy = lax.axis_index("gx"), lax.axis_index("gy")
    left, right = (lax.rem(gx + nx - 1, nx), gy), (lax.rem(gx + 1, nx), gy)
    down, up = (gx, lax.rem(gy + ny - 1, ny)), (gx, lax.rem(gy + 1, ny))
    half = slots // 2
    per = half // CHUNKS

    loads = [
        pltpu.make_async_copy(src, dst, in_sem.at[i])
        for i, (src, dst) in enumerate(
            [(drops_hbm, cur.at[0]), (moves_hbm, moves), (order_hbm, order), (tries_hbm, tries)]
        )
    ]
    for load in loads:
        load.start()

    barrier = pltpu.get_barrier_semaphore()
    for d in range(1, nx):
        pl.semaphore_signal(barrier, inc=1, device_id=(lax.rem(gx + d, nx), gy), device_id_type=MESH)
    for d in range(1, ny):
        pl.semaphore_signal(barrier, inc=1, device_id=(gx, lax.rem(gy + d, ny)), device_id_type=MESH)

    row = lax.broadcasted_iota(jnp.int32, (ROWS, LANES), 0)
    lane = lax.broadcasted_iota(jnp.int32, (ROWS, LANES), 1)
    even = lax.rem(row, 2) == 0
    group = lane // LEVELS
    groups = LANES // LEVELS

    def remote(src, dst, ss, rs, dev):
        return pltpu.make_async_remote_copy(
            src_ref=src, dst_ref=dst, send_sem=ss, recv_sem=rs, device_id=dev, device_id_type=MESH
        )

    def chunk_slots(q):
        return [q * per + t for t in range(per)] + [half + q * per + t for t in range(per)]

    def pack_chunk(step, q):
        for v in range(2):
            for t in range(per):
                a, b = cur[step, v, q * per + t], cur[step, v, half + q * per + t]
                send_r[step, q, v, t] = jnp.where(even, roll(a, -1, 0), b)
                send_l[step, q, v, t] = jnp.where(even, a, roll(b, 1, 0))

    def x_copies(step, q):
        return [
            remote(send_r.at[step, q], halo_l.at[step, q], xs_sem.at[step, 0, q], xl_sem.at[step, q], right),
            remote(send_l.at[step, q], halo_r.at[step, q], xs_sem.at[step, 1, q], xr_sem.at[step, q], left),
        ]

    def send_state(step):
        for q in range(CHUNKS):
            pack_chunk(step, q)
        copies = []
        for q in range(CHUNKS):
            pair = x_copies(step, q)
            for c in pair:
                c.start()
            copies.append(pair)
        return copies

    loads[0].wait()
    for q in range(CHUNKS):
        pack_chunk(0, q)
    loads[1].wait()
    for step in range(steps):
        packed = jnp.zeros((ROWS, LANES), jnp.int32)
        for q in range(CHUNKS):
            part = jnp.zeros((ROWS, LANES), jnp.int32)
            for g, s in enumerate(chunk_slots(q)):
                part = jnp.where(group == g, roll(moves[step, s], LEVELS * g, 1), part)
            packed = jnp.where(row // 2 == q, roll(part, 2 * q, 0), packed)
        code_send[step] = packed
    pl.semaphore_wait(barrier, nx + ny - 2)
    code_copies = [
        remote(code_send, code_l, cs_sem.at[0], cl_sem, right),
        remote(code_send, code_r, cs_sem.at[1], cr_sem, left),
    ]
    for c in code_copies:
        c.start()
    copies = []
    for q in range(CHUNKS):
        pair = x_copies(0, q)
        for c in pair:
            c.start()
        copies.append(pair)

    for c in code_copies:
        c.wait()
    for step in range(steps):
        own = code_send[step]
        swapped = jnp.where(even, roll(own, -1, 0), roll(own, 1, 0))
        outer = jnp.where(even, roll(code_l[step], -1, 0), roll(code_r[step], 1, 0))
        from_halo = jnp.where(even, own, 8 - own) >= 6
        landed = jnp.where((own >= 3) & (own < 6), own, jnp.where(from_halo, outer, swapped))
        y_step = lax.rem(landed, 3) - 1
        for q in range(CHUNKS):
            lift = roll(y_step, -2 * q, 0)
            lift = jnp.where(row < 2, lift, 0)
            lift = lift + roll(lift, 2, 0)
            lift = lift + roll(lift, 4, 0)
            for g, s in enumerate(chunk_slots(q)):
                one = jnp.where(group == 0, roll(lift, -LEVELS * g, 1), 0)
                width = LEVELS
                while width < LANES:
                    one = one + roll(one, width, 1)
                    width *= 2
                cy_ref[step, s] = one

    row_totals = []
    loads[2].wait()
    loads[3].wait()
    for step in range(steps):
        edge_copies = []
        for q in range(CHUNKS):
            for c in copies[q]:
                c.wait()
            members = chunk_slots(q)
            for v in range(2):
                packed = jnp.zeros((ROWS, LANES), jnp.float32)
                for g, s in enumerate(members):
                    t = g % per
                    hl, hr = halo_l[step, q, v, t], halo_r[step, q, v, t]
                    if g < per:
                        outer = jnp.where(even, hl, roll(hr, 1, 0))
                    else:
                        outer = jnp.where(even, roll(hl, -1, 0), hr)
                    mine, code = cur[step, v, s], moves[step, s]
                    swapped = jnp.where(even, roll(mine, -1, 0), roll(mine, 1, 0))
                    from_halo = jnp.where(even, code, 8 - code) >= 6
                    new = jnp.where(
                        (code >= 3) & (code < 6), mine, jnp.where(from_halo, outer, swapped)
                    )
                    moved[v, s] = new
                    edges = jnp.where(row < 2, new, roll(new, LEVELS, 1))
                    packed = jnp.where(group == g, roll(edges, LEVELS * g, 1), packed)
                edge_send[step, q, v] = packed
            sends = [remote(edge_send.at[step, q], edge_dn.at[step, q], es_sem.at[step, 0, q], ed_sem.at[step, q], up)]
            if ny > 2:
                sends.append(
                    remote(edge_send.at[step, q], edge_up.at[step, q], es_sem.at[step, 1, q], eu_sem.at[step, q], down)
                )
            for c in sends:
                c.start()
            edge_copies.append(sends)
        for q in range(CHUNKS):
            for c in edge_copies[q]:
                c.wait()
            above = edge_up if ny > 2 else edge_dn
            for v in range(2):
                low, high = edge_dn[step, q, v], above[step, q, v]
                for g, s in enumerate(chunk_slots(q)):
                    mine, dy = moved[v, s], cy_ref[step, s]
                    fwd, bwd = roll(mine, LEVELS, 1), roll(mine, -LEVELS, 1)
                    fwd_in = roll(jnp.where(row >= ROWS - 2, roll(low, -LEVELS * g, 1), fwd), 2, 0)
                    bwd_in = roll(jnp.where(row < 2, roll(high, -LEVELS * (g + 1), 1), bwd), -2, 0)
                    fwd = jnp.where(group == 0, fwd_in, fwd)
                    bwd = jnp.where(group == groups - 1, bwd_in, bwd)
                    moved[v, s] = jnp.where(dy == 0, mine, jnp.where(dy > 0, fwd, bwd))

        def pair_body(i, _):
            found = []
            for k in range(2):
                index = order[step, 2 * i + k]
                bits = [(index & (1 << b)) != 0 for b in range((slots - 1).bit_length())]
                for v in range(2):
                    found.append(tree([moved[v, s] for s in range(slots)], bits))
            na, ma, nb, mb = found
            na, nb, ma, mb = collide(na, nb, ma, mb, tries[step, i])
            paired[0, 2 * i] = na
            paired[0, 2 * i + 1] = nb
            paired[1, 2 * i] = ma
            paired[1, 2 * i + 1] = mb
            return 0

        lax.fori_loop(0, half, pair_body, 0)

        width = 8

        def slot_body(i, sums):
            base = i * width
            counts = [jnp.zeros((ROWS, LANES), jnp.float32)] * width
            masses = [jnp.zeros((ROWS, LANES), jnp.float32)] * width
            for p in range(slots):
                index = order[step, p] - base
                pn, pm = paired[0, p], paired[1, p]
                for k in range(width):
                    hit = index == k
                    counts[k] = jnp.where(hit, pn, counts[k])
                    masses[k] = jnp.where(hit, pm, masses[k])
            count, liquid = sums
            for k in range(width):
                cur[step + 1, 0, base + k] = counts[k]
                cur[step + 1, 1, base + k] = masses[k]
                count = count + counts[k]
                liquid = liquid + counts[k] * masses[k]
            return count, liquid

        zero = jnp.zeros((ROWS, LANES), jnp.float32)
        sums = lax.fori_loop(0, slots // width, slot_body, (zero, zero))
        if step + 1 < steps:
            copies = send_state(step + 1)
        for total in sums:
            shift = ROWS // 2
            while shift:
                total = total + roll(total, shift, 0)
                shift //= 2
            shift = LANES // 2
            while shift >= LEVELS:
                total = total + roll(total, shift, 1)
                shift //= 2
            row_totals.append(total)

    result = pltpu.make_async_copy(cur.at[steps], out_hbm, out_sem)
    result.start()

    mine = row_totals[0]
    for i in range(1, len(row_totals)):
        mine = jnp.where(group == i, row_totals[i], mine)

    def gather_sum(value, part, got, ss, rs, me, size, peer):
        part[...] = value
        sends = [
            remote(part, got.at[d - 1], ss.at[d - 1], rs.at[d - 1], peer(lax.rem(me + d, size)))
            for d in range(1, size)
        ]
        for c in sends:
            c.start()
        for c in sends:
            c.wait()
        total = jnp.zeros_like(value)
        for i in range(size):
            term = jnp.where(me == i, 1.0, 0.0) * value
            for d in range(1, size):
                term = term + jnp.where(lax.rem(me + size - d, size) == i, 1.0, 0.0) * got[d - 1]
            total = total + term
        return total

    mine = gather_sum(mine, part_y, got_y, ys_sem, yr_sem, gy, ny, lambda p: (gx, p))
    part_x[...] = mine
    sends = []
    for d in range(1, nx):
        c = remote(part_x, got_x.at[gx], gs_sem.at[d - 1], gr_sem.at[d - 1], (lax.rem(gx + d, nx), gy))
        c.start()
        sends.append(c)
    got_x[gx] = mine
    for c in sends:
        c.wait()
    total = got_x[0]
    for i in range(1, nx):
        total = total + got_x[i]
    total = total * scale
    for i in range(steps):
        for v in range(2):
            mom_ref[i, v : v + 1, :] = roll(total, -LEVELS * (2 * i + v), 1)[0:1, :LEVELS]
    result.wait()


def solution(mesh):
    nx, ny = mesh.shape["gx"], mesh.shape["gy"]

    def body(droplets, moves, pairing, collisions):
        two, slots, cols, flat = droplets.shape
        steps, tiles = moves.shape[0], flat // LANES
        assert cols * tiles == ROWS and cols == 2

        def view(a):
            lead = a.shape[:2]
            return a.reshape(*lead, cols, tiles, LANES).swapaxes(2, 3).reshape(*lead, ROWS, LANES)

        f32, i32 = jnp.float32, jnp.int32
        tile = (ROWS, LANES)
        per = slots // 2 // CHUNKS
        dma = pltpu.SemaphoreType.DMA
        halo = pltpu.VMEM((steps, CHUNKS, 2, per, *tile), f32)
        edge = pltpu.VMEM((steps, CHUNKS, 2, *tile), f32)
        code = pltpu.VMEM((steps, *tile), i32)
        scale = 1.0 / (cols * nx * (flat // LEVELS) * ny * count_unit)
        any_space = pl.BlockSpec(memory_space=pl.ANY)
        out, moments = pl.pallas_call(
            functools.partial(kernel, nx, ny, slots, steps, scale),
            out_shape=(
                jax.ShapeDtypeStruct((two, slots, *tile), f32),
                jax.ShapeDtypeStruct((steps, 2, LEVELS), f32),
            ),
            in_specs=[any_space] * 4,
            out_specs=(any_space, pl.BlockSpec(memory_space=pltpu.VMEM)),
            scratch_shapes=[
                pltpu.VMEM((steps + 1, two, slots, *tile), f32),
                pltpu.VMEM((steps, slots, *tile), i32),
                pltpu.VMEM((steps, slots, *tile), i32),
                pltpu.VMEM((steps, slots // 2, *tile), i32),
                pltpu.VMEM((two, slots, *tile), f32),
                pltpu.VMEM((two, slots, *tile), f32),
                pltpu.VMEM((steps, slots, *tile), i32),
                halo, halo, halo, halo,
                code, code, code,
                edge, edge, edge,
                pltpu.VMEM(tile, f32),
                pltpu.VMEM((ny - 1, *tile), f32),
                pltpu.VMEM(tile, f32),
                pltpu.VMEM((nx, *tile), f32),
                dma((4,)), dma,
                dma((steps, 2, CHUNKS)), dma((steps, CHUNKS)), dma((steps, CHUNKS)),
                dma((2,)), dma, dma,
                dma((steps, 2, CHUNKS)), dma((steps, CHUNKS)), dma((steps, CHUNKS)),
                dma((ny - 1,)), dma((ny - 1,)), dma((nx - 1,)), dma((nx - 1,)),
            ],
            compiler_params=pltpu.CompilerParams(collective_id=0, has_side_effects=True),
        )(view(droplets), view(moves), view(pairing), view(collisions))
        out = out.reshape(two, slots, tiles, cols, LANES).swapaxes(2, 3).reshape(droplets.shape)
        return out, moments

    placed = P(None, None, "gx", "gy")
    return jax.shard_map(
        body, mesh=mesh, in_specs=(placed,) * 4, out_specs=(placed, P()), check_vma=False
    )
```

```python
import functools

import jax
import jax.numpy as jnp
from jax import lax
from jax.experimental import pallas as pl
from jax.experimental.pallas import tpu as pltpu
from jax.sharding import PartitionSpec as P

LEVELS = 16
LANES = 128
ROWS = 8
CHUNKS = 4
count_unit = 4096.0
MESH = pl.DeviceIdType.MESH


def roll(value, shift, axis):
    shift = shift % value.shape[axis]
    return value if shift == 0 else pltpu.roll(value, shift, axis)


def tree(values, bits):
    level = 0
    while len(values) > 1:
        values = [
            jnp.where(bits[level], values[i + 1], values[i]) for i in range(0, len(values), 2)
        ]
        level += 1
    return values[0]


def collide(na, nb, ma, mb, tries):
    first = na >= nb
    big, small = jnp.maximum(na, nb), jnp.minimum(na, nb)
    big_m, small_m = jnp.where(first, ma, mb), jnp.where(first, mb, ma)
    most = jnp.where(3.0 * small <= big, 3.0, jnp.where(2.0 * small <= big, 2.0, 1.0))
    taken = jnp.minimum(tries.astype(jnp.float32), most)
    remain = big - taken * small
    split = remain == 0.0
    half = jnp.floor(small * 0.5)
    big_new = jnp.where(split, half, remain)
    small_new = jnp.where(split, small - half, small)
    grown = small_m + taken * big_m
    big_m_new = jnp.where(split, grown, big_m)
    return (
        jnp.where(first, big_new, small_new),
        jnp.where(first, small_new, big_new),
        jnp.where(first, big_m_new, grown),
        jnp.where(first, grown, big_m_new),
    )


def kernel(
    nx, ny, slots, steps, scale,
    drops_hbm, moves_hbm, order_hbm, tries_hbm, out_ref, mom_ref,
    cur, moves, order, tries, moved, paired, cy_ref,
    send_l, send_r, halo_l, halo_r,
    code_send, code_l, code_r,
    rim, rim_l, rim_r, rim_code, edge_send, edge_dn, edge_up,
    in_sem, xs_sem, xl_sem, xr_sem, cs_sem, cl_sem, cr_sem,
    rs_sem, rl_sem, rr_sem, es_sem, ed_sem, eu_sem, *sums_refs,
):
    gx, gy = lax.axis_index("gx"), lax.axis_index("gy")
    left, right = (lax.rem(gx + nx - 1, nx), gy), (lax.rem(gx + 1, nx), gy)
    down, up = (gx, lax.rem(gy + ny - 1, ny)), (gx, lax.rem(gy + 1, ny))
    width = slots // CHUNKS
    per = width // 2
    stages = sum_stages(nx, ny, gx, gy)

    barrier = pltpu.get_barrier_semaphore()
    greeted = 0
    for size, me, device in stages:
        for d in range(1, size):
            pl.semaphore_signal(barrier, inc=1, device_id=device(lax.rem(me + d, size)), device_id_type=MESH)
        greeted += size - 1

    loads = [
        pltpu.make_async_copy(src, dst, in_sem.at[i])
        for i, (src, dst) in enumerate(
            [(drops_hbm, cur.at[0]), (moves_hbm, moves), (order_hbm, order), (tries_hbm, tries)]
        )
    ]
    for load in loads:
        load.start()

    row = lax.broadcasted_iota(jnp.int32, (ROWS, LANES), 0)
    lane = lax.broadcasted_iota(jnp.int32, (ROWS, LANES), 1)
    even = lax.rem(row, 2) == 0
    group = lane // LEVELS
    groups = LANES // LEVELS

    def remote(src, dst, ss, rs, dev):
        return pltpu.make_async_remote_copy(
            src_ref=src, dst_ref=dst, send_sem=ss, recv_sem=rs, device_id=dev, device_id_type=MESH
        )

    def x_copies(step, q):
        return [
            remote(send_r.at[step, q], halo_l.at[step, q], xs_sem.at[step, 0, q], xl_sem.at[step, q], right),
            remote(send_l.at[step, q], halo_r.at[step, q], xs_sem.at[step, 1, q], xr_sem.at[step, q], left),
        ]

    def rim_copies(step):
        return [
            remote(rim.at[step, 1], rim_l.at[step], rs_sem.at[step, 0], rl_sem.at[step], right),
            remote(rim.at[step, 0], rim_r.at[step], rs_sem.at[step, 1], rr_sem.at[step], left),
        ]

    def start(copies):
        for c in copies:
            c.start()

    def wait(copies):
        for c in copies:
            c.wait()

    def pack_sides(step, q, v, values):
        for t in range(per):
            a, b = values[t], values[per + t]
            send_r[step, q, v, t] = jnp.where(even, roll(a, -1, 0), b)
            send_l[step, q, v, t] = jnp.where(even, a, roll(b, 1, 0))

    def pack_rim(values):
        packed = jnp.zeros((ROWS, LANES), values[0].dtype)
        for g, value in enumerate(values):
            ends = jnp.where(row < 2, value, roll(value, LEVELS, 1))
            packed = jnp.where(group == g, roll(ends, LEVELS * g, 1), packed)
        return packed

    def store_rim(step, q, v, values):
        packed = pack_rim(values)
        for c in range(2):
            rim[step, c, v, pl.ds(2 * q, 1), :] = packed[c : c + 1]
            rim[step, c, v, pl.ds(2 * q + 1, 1), :] = packed[ROWS - 2 + c : ROWS - 1 + c]

    loads[1].wait()
    for step in range(steps):
        packed = jnp.zeros((ROWS, LANES), jnp.int32)
        for q in range(CHUNKS):
            part = pack_rim([moves[step, q * width + g] for g in range(width)])
            packed = jnp.where(row // 2 == q, roll(part, 2 * q, 0), packed)
            rim_code[step, 2 * q : 2 * q + 1, :] = part[0:1]
            rim_code[step, 2 * q + 1 : 2 * q + 2, :] = part[ROWS - 2 : ROWS - 1]
        code_send[step] = packed
    loads[0].wait()
    for q in range(CHUNKS):
        for v in range(2):
            values = [cur[0, v, q * width + g] for g in range(width)]
            store_rim(0, q, v, values)
            pack_sides(0, q, v, values)
    pl.semaphore_wait(barrier, greeted)
    code_copies = [
        remote(code_send, code_l, cs_sem.at[0], cl_sem, right),
        remote(code_send, code_r, cs_sem.at[1], cr_sem, left),
    ]
    start(rim_copies(0))
    start(code_copies)
    for q in range(CHUNKS):
        start(x_copies(0, q))

    def edge_copies(step):
        out = [remote(edge_send.at[step], edge_dn.at[step], es_sem.at[step, 0], ed_sem.at[step], up)]
        if ny > 2:
            out.append(remote(edge_send.at[step], edge_up.at[step], es_sem.at[step, 1], eu_sem.at[step], down))
        return out

    def send_edges(step):
        wait(rim_copies(step))
        code = rim_code[step]
        for v in range(2):
            first, last = rim[step, 0, v], rim[step, 1, v]
            before, after = rim_l[step, v], rim_r[step, v]
            stay, ahead = (code >= 3) & (code < 6), code >= 6
            edge_send[step, 0, v] = jnp.where(stay, first, jnp.where(ahead, before, last))
            edge_send[step, 1, v] = jnp.where(stay, last, jnp.where(ahead, first, after))
        start(edge_copies(step))

    send_edges(0)
    wait(code_copies)
    for step in range(steps):
        own = code_send[step]
        swapped = jnp.where(even, roll(own, -1, 0), roll(own, 1, 0))
        outer = jnp.where(even, roll(code_l[step], -1, 0), roll(code_r[step], 1, 0))
        from_halo = jnp.where(even, own, 8 - own) >= 6
        landed = jnp.where((own >= 3) & (own < 6), own, jnp.where(from_halo, outer, swapped))
        y_step = lax.rem(landed, 3) - 1
        for q in range(CHUNKS):
            lift = roll(y_step, -2 * q, 0)
            lift = jnp.where(row < 2, lift, 0)
            lift = lift + roll(lift, 2, 0)
            lift = lift + roll(lift, 4, 0)
            for g in range(width):
                one = jnp.where(group == 0, roll(lift, -LEVELS * g, 1), 0)
                span = LEVELS
                while span < LANES:
                    one = one + roll(one, span, 1)
                    span *= 2
                cy_ref[step, q * width + g] = one

    row_totals = []
    for step in range(steps):
        if step:
            send_edges(step)
        wait(edge_copies(step))
        above = edge_up if ny > 2 else edge_dn
        for q in range(CHUNKS):
            wait(x_copies(step, q))
            for v in range(2):
                low = jnp.where(
                    even, edge_dn[step, 0, v, 2 * q + 1 : 2 * q + 2, :], edge_dn[step, 1, v, 2 * q + 1 : 2 * q + 2, :]
                )
                high = jnp.where(
                    even, above[step, 0, v, 2 * q : 2 * q + 1, :], above[step, 1, v, 2 * q : 2 * q + 1, :]
                )
                for g in range(width):
                    s, t = q * width + g, g % per
                    hl, hr = halo_l[step, q, v, t], halo_r[step, q, v, t]
                    if g < per:
                        outer = jnp.where(even, hl, roll(hr, 1, 0))
                    else:
                        outer = jnp.where(even, roll(hl, -1, 0), hr)
                    mine, code = cur[step, v, s], moves[step, s]
                    swapped = jnp.where(even, roll(mine, -1, 0), roll(mine, 1, 0))
                    from_halo = jnp.where(even, code, 8 - code) >= 6
                    mine = jnp.where(
                        (code >= 3) & (code < 6), mine, jnp.where(from_halo, outer, swapped)
                    )
                    dy = cy_ref[step, s]
                    fwd, bwd = roll(mine, LEVELS, 1), roll(mine, -LEVELS, 1)
                    fwd_in = jnp.where(row < 2, roll(low, -LEVELS * g, 1), roll(fwd, 2, 0))
                    bwd_in = jnp.where(row >= ROWS - 2, roll(high, -LEVELS * (g + 1), 1), roll(bwd, -2, 0))
                    fwd = jnp.where(group == 0, fwd_in, fwd)
                    bwd = jnp.where(group == groups - 1, bwd_in, bwd)
                    moved[v, s] = jnp.where(dy == 0, mine, jnp.where(dy > 0, fwd, bwd))
        if step == 0:
            wait(loads[2:])

        def pair_body(i, _):
            found = []
            for k in range(2):
                index = order[step, 2 * i + k]
                bits = [(index & (1 << b)) != 0 for b in range((slots - 1).bit_length())]
                for v in range(2):
                    found.append(tree([moved[v, s] for s in range(slots)], bits))
            na, ma, nb, mb = found
            na, nb, ma, mb = collide(na, nb, ma, mb, tries[step, i])
            paired[0, 2 * i] = na
            paired[0, 2 * i + 1] = nb
            paired[1, 2 * i] = ma
            paired[1, 2 * i + 1] = mb
            return 0

        lax.fori_loop(0, slots // 2, pair_body, 0)

        def slot_body(q, sums):
            base = q * width
            counts = [jnp.zeros((ROWS, LANES), jnp.float32)] * width
            masses = [jnp.zeros((ROWS, LANES), jnp.float32)] * width
            for p in range(slots):
                index = order[step, p] - base
                pn, pm = paired[0, p], paired[1, p]
                for k in range(width):
                    hit = index == k
                    counts[k] = jnp.where(hit, pn, counts[k])
                    masses[k] = jnp.where(hit, pm, masses[k])
            if step + 1 < steps:
                pack_sides(step + 1, q, 0, counts)
                pack_sides(step + 1, q, 1, masses)
            count, liquid = sums
            target = cur.at[step + 1] if step + 1 < steps else out_ref
            for k in range(width):
                target[0, base + k] = counts[k]
                target[1, base + k] = masses[k]
                count = count + counts[k]
                liquid = liquid + counts[k] * masses[k]
            if step + 1 < steps:
                store_rim(step + 1, q, 0, counts)
                store_rim(step + 1, q, 1, masses)
                start(x_copies(step + 1, q))
            return count, liquid

        zero = jnp.zeros((ROWS, LANES), jnp.float32)
        sums = lax.fori_loop(0, CHUNKS, slot_body, (zero, zero))
        if step + 1 < steps:
            start(rim_copies(step + 1))
        for total in sums:
            shift = ROWS // 2
            while shift:
                total = total + roll(total, shift, 0)
                shift //= 2
            shift = LANES // 2
            while shift >= LEVELS:
                total = total + roll(total, shift, 1)
                shift //= 2
            row_totals.append(total)

    total = row_totals[0]
    for i in range(1, len(row_totals)):
        total = jnp.where(group == i, row_totals[i], total)
    total = total[0:1]
    for k, (size, me, device) in enumerate(stages):
        part, got, ss, rs = sums_refs[4 * k : 4 * k + 4]
        part[...] = total
        got[me] = total
        sends = [
            remote(part, got.at[me], ss.at[d - 1], rs.at[d - 1], device(lax.rem(me + d, size)))
            for d in range(1, size)
        ]
        start(sends)
        wait(sends)
        terms = [got[i] for i in range(size)]
        while len(terms) > 1:
            terms = [sum(terms[i + 1 : i + 2], terms[i]) for i in range(0, len(terms), 2)]
        total = terms[0]
    total = jnp.broadcast_to(total * scale, (ROWS, LANES))
    for i in range(steps):
        for v in range(2):
            mom_ref[i, v : v + 1, :] = roll(total, -LEVELS * (2 * i + v), 1)[0:1, :LEVELS]


def sum_stages(nx, ny, gx, gy):
    if nx * ny <= 64:
        return [(nx * ny, gx * ny + gy, lambda p: (p // ny, lax.rem(p, ny)))]
    return [(ny, gy, lambda p: (gx, p)), (nx, gx, lambda p: (p, gy))]


def solution(mesh):
    nx, ny = mesh.shape["gx"], mesh.shape["gy"]

    def body(droplets, moves, pairing, collisions):
        two, slots, cols, flat = droplets.shape
        steps, tiles = moves.shape[0], flat // LANES
        assert cols * tiles == ROWS and cols == 2

        def view(a):
            lead = a.shape[:2]
            return a.reshape(*lead, cols, tiles, LANES).swapaxes(2, 3).reshape(*lead, ROWS, LANES)

        f32, i32 = jnp.float32, jnp.int32
        tile = (ROWS, LANES)
        per = slots // 2 // CHUNKS
        dma = pltpu.SemaphoreType.DMA
        halo = pltpu.VMEM((steps, CHUNKS, 2, per, *tile), f32)
        edge = pltpu.VMEM((steps, 2, 2, *tile), f32)
        rim = pltpu.VMEM((steps, 2, *tile), f32)
        sums = []
        for size, _, _ in sum_stages(nx, ny, 0, 0):
            sums += [pltpu.VMEM((1, LANES), f32), pltpu.VMEM((size, 1, LANES), f32), dma((size - 1,)), dma((size - 1,))]
        code = pltpu.VMEM((steps, *tile), i32)
        scale = 1.0 / (cols * nx * (flat // LEVELS) * ny * count_unit)
        any_space = pl.BlockSpec(memory_space=pl.ANY)
        out, moments = pl.pallas_call(
            functools.partial(kernel, nx, ny, slots, steps, scale),
            out_shape=(
                pltpu.VMEM((two, slots, *tile), f32),
                jax.ShapeDtypeStruct((steps, 2, LEVELS), f32),
            ),
            in_specs=[any_space] * 4,
            out_specs=(pl.BlockSpec(memory_space=pltpu.VMEM), pl.BlockSpec(memory_space=pltpu.VMEM)),
            scratch_shapes=[
                pltpu.VMEM((steps, two, slots, *tile), f32),
                pltpu.VMEM((steps, slots, *tile), i32),
                pltpu.VMEM((steps, slots, *tile), i32),
                pltpu.VMEM((steps, slots // 2, *tile), i32),
                pltpu.VMEM((two, slots, *tile), f32),
                pltpu.VMEM((two, slots, *tile), f32),
                pltpu.VMEM((steps, slots, *tile), i32),
                halo, halo, halo, halo,
                code, code, code,
                edge, rim, rim, code, edge, edge, edge,
                dma((4,)),
                dma((steps, 2, CHUNKS)), dma((steps, CHUNKS)), dma((steps, CHUNKS)),
                dma((2,)), dma, dma,
                dma((steps, 2)), dma((steps,)), dma((steps,)),
                dma((steps, 2)), dma((steps,)), dma((steps,)),
                *sums,
            ],
            compiler_params=pltpu.CompilerParams(collective_id=0, has_side_effects=True),
        )(view(droplets), view(moves), view(pairing), view(collisions))
        out = out.reshape(two, slots, tiles, cols, LANES).swapaxes(2, 3).reshape(droplets.shape)
        return out, moments

    placed = P(None, None, "gx", "gy")
    return jax.shard_map(
        body, mesh=mesh, in_specs=(placed,) * 4, out_specs=(placed, P()), check_vma=False
    )
```

```python
import functools

import jax
import jax.numpy as jnp
from jax import lax
from jax.experimental import pallas as pl
from jax.experimental.pallas import tpu as pltpu
from jax.sharding import PartitionSpec as P

LEVELS = 16
LANES = 128
ROWS = 8
CHUNKS = 4
count_unit = 4096.0
MESH = pl.DeviceIdType.MESH


def roll(value, shift, axis):
    shift = shift % value.shape[axis]
    return value if shift == 0 else pltpu.roll(value, shift, axis)


def tree(values, bits):
    level = 0
    while len(values) > 1:
        values = [
            jnp.where(bits[level], values[i + 1], values[i]) for i in range(0, len(values), 2)
        ]
        level += 1
    return values[0]


def collide(na, nb, ma, mb, tries):
    first = na >= nb
    big, small = jnp.maximum(na, nb), jnp.minimum(na, nb)
    big_m, small_m = jnp.where(first, ma, mb), jnp.where(first, mb, ma)
    most = jnp.where(3.0 * small <= big, 3.0, jnp.where(2.0 * small <= big, 2.0, 1.0))
    taken = jnp.minimum(tries.astype(jnp.float32), most)
    remain = big - taken * small
    split = remain == 0.0
    half = jnp.floor(small * 0.5)
    big_new = jnp.where(split, half, remain)
    small_new = jnp.where(split, small - half, small)
    grown = small_m + taken * big_m
    big_m_new = jnp.where(split, grown, big_m)
    return (
        jnp.where(first, big_new, small_new),
        jnp.where(first, small_new, big_new),
        jnp.where(first, big_m_new, grown),
        jnp.where(first, grown, big_m_new),
    )


def kernel(
    nx, ny, slots, steps, scale,
    drops_hbm, moves_hbm, order_hbm, tries_hbm, out_ref, mom_ref,
    cur, moves, order, tries, moved, paired, cy_ref,
    send_l, send_r, halo_l, halo_r,
    code_send, code_l, code_r,
    rim, rim_l, rim_r, rim_code, edge_send, edge_dn, edge_up,
    in_sem, xs_sem, xl_sem, xr_sem, cs_sem, cl_sem, cr_sem,
    rs_sem, rl_sem, rr_sem, es_sem, ed_sem, eu_sem, *sums_refs,
):
    gx, gy = lax.axis_index("gx"), lax.axis_index("gy")
    left, right = (lax.rem(gx + nx - 1, nx), gy), (lax.rem(gx + 1, nx), gy)
    down, up = (gx, lax.rem(gy + ny - 1, ny)), (gx, lax.rem(gy + 1, ny))
    width = slots // CHUNKS
    per = width // 2
    stages = sum_stages(nx, ny, gx, gy)

    barrier = pltpu.get_barrier_semaphore()
    greeted = 0
    for size, me, device in stages:
        for d in range(1, size):
            pl.semaphore_signal(barrier, inc=1, device_id=device(lax.rem(me + d, size)), device_id_type=MESH)
        greeted += size - 1

    loads = [
        pltpu.make_async_copy(src, dst, in_sem.at[i])
        for i, (src, dst) in enumerate(
            [(drops_hbm, cur.at[0]), (moves_hbm, moves), (order_hbm, order), (tries_hbm, tries)]
        )
    ]
    for load in loads:
        load.start()

    row = lax.broadcasted_iota(jnp.int32, (ROWS, LANES), 0)
    lane = lax.broadcasted_iota(jnp.int32, (ROWS, LANES), 1)
    even = lax.rem(row, 2) == 0
    group = lane // LEVELS
    groups = LANES // LEVELS

    def remote(src, dst, ss, rs, dev):
        return pltpu.make_async_remote_copy(
            src_ref=src, dst_ref=dst, send_sem=ss, recv_sem=rs, device_id=dev, device_id_type=MESH
        )

    def x_copies(step, q):
        return [
            remote(send_r.at[step, q], halo_l.at[step, q], xs_sem.at[step, 0, q], xl_sem.at[step, q], right),
            remote(send_l.at[step, q], halo_r.at[step, q], xs_sem.at[step, 1, q], xr_sem.at[step, q], left),
        ]

    def rim_copies(step):
        return [
            remote(rim.at[step, 1], rim_l.at[step], rs_sem.at[step, 0], rl_sem.at[step], right),
            remote(rim.at[step, 0], rim_r.at[step], rs_sem.at[step, 1], rr_sem.at[step], left),
        ]

    def start(copies):
        for c in copies:
            c.start()

    def wait(copies):
        for c in copies:
            c.wait()

    def pack_sides(step, q, v, values):
        for t in range(per):
            a, b = values[t], values[per + t]
            send_r[step, q, v, t] = jnp.where(even, roll(a, -1, 0), b)
            send_l[step, q, v, t] = jnp.where(even, a, roll(b, 1, 0))

    def pack_rim(values):
        packed = jnp.zeros((ROWS, LANES), values[0].dtype)
        for g, value in enumerate(values):
            ends = jnp.where(row < 2, value, roll(value, LEVELS, 1))
            packed = jnp.where(group == g, roll(ends, LEVELS * g, 1), packed)
        return packed

    def store_rim(step, q, v, values):
        packed = pack_rim(values)
        for c in range(2):
            rim[step, c, v, pl.ds(2 * q, 1), :] = packed[c : c + 1]
            rim[step, c, v, pl.ds(2 * q + 1, 1), :] = packed[ROWS - 2 + c : ROWS - 1 + c]

    loads[1].wait()
    for step in range(steps):
        packed = jnp.zeros((ROWS, LANES), jnp.int32)
        for q in range(CHUNKS):
            part = pack_rim([moves[step, q * width + g] for g in range(width)])
            packed = jnp.where(row // 2 == q, roll(part, 2 * q, 0), packed)
            rim_code[step, 2 * q : 2 * q + 1, :] = part[0:1]
            rim_code[step, 2 * q + 1 : 2 * q + 2, :] = part[ROWS - 2 : ROWS - 1]
        code_send[step] = packed
    loads[0].wait()
    for q in range(CHUNKS):
        for v in range(2):
            values = [cur[0, v, q * width + g] for g in range(width)]
            store_rim(0, q, v, values)
            pack_sides(0, q, v, values)
    pl.semaphore_wait(barrier, greeted)
    code_copies = [
        remote(code_send, code_l, cs_sem.at[0], cl_sem, right),
        remote(code_send, code_r, cs_sem.at[1], cr_sem, left),
    ]
    start(rim_copies(0))
    start(code_copies)
    for q in range(CHUNKS):
        start(x_copies(0, q))

    def edge_copies(step):
        out = [remote(edge_send.at[step], edge_dn.at[step], es_sem.at[step, 0], ed_sem.at[step], up)]
        if ny > 2:
            out.append(remote(edge_send.at[step], edge_up.at[step], es_sem.at[step, 1], eu_sem.at[step], down))
        return out

    def send_edges(step):
        wait(rim_copies(step))
        code = rim_code[step]
        for v in range(2):
            first, last = rim[step, 0, v], rim[step, 1, v]
            before, after = rim_l[step, v], rim_r[step, v]
            stay, ahead = (code >= 3) & (code < 6), code >= 6
            edge_send[step, 0, v] = jnp.where(stay, first, jnp.where(ahead, before, last))
            edge_send[step, 1, v] = jnp.where(stay, last, jnp.where(ahead, first, after))
        start(edge_copies(step))

    send_edges(0)
    wait(code_copies)
    for step in range(steps):
        own = code_send[step]
        swapped = jnp.where(even, roll(own, -1, 0), roll(own, 1, 0))
        outer = jnp.where(even, roll(code_l[step], -1, 0), roll(code_r[step], 1, 0))
        from_halo = jnp.where(even, own, 8 - own) >= 6
        landed = jnp.where((own >= 3) & (own < 6), own, jnp.where(from_halo, outer, swapped))
        y_step = lax.rem(landed, 3) - 1
        for q in range(CHUNKS):
            lift = roll(y_step, -2 * q, 0)
            lift = jnp.where(row < 2, lift, 0)
            lift = lift + roll(lift, 2, 0)
            lift = lift + roll(lift, 4, 0)
            for g in range(width):
                one = jnp.where(group == 0, roll(lift, -LEVELS * g, 1), 0)
                span = LEVELS
                while span < LANES:
                    one = one + roll(one, span, 1)
                    span *= 2
                cy_ref[step, q * width + g] = one

    row_totals = []
    for step in range(steps):
        if step:
            send_edges(step)
        wait(edge_copies(step))
        above = edge_up if ny > 2 else edge_dn
        for q in range(CHUNKS):
            wait(x_copies(step, q))
            for v in range(2):
                low = jnp.where(
                    even, edge_dn[step, 0, v, 2 * q + 1 : 2 * q + 2, :], edge_dn[step, 1, v, 2 * q + 1 : 2 * q + 2, :]
                )
                high = jnp.where(
                    even, above[step, 0, v, 2 * q : 2 * q + 1, :], above[step, 1, v, 2 * q : 2 * q + 1, :]
                )
                for g in range(width):
                    s, t = q * width + g, g % per
                    hl, hr = halo_l[step, q, v, t], halo_r[step, q, v, t]
                    if g < per:
                        outer = jnp.where(even, hl, roll(hr, 1, 0))
                    else:
                        outer = jnp.where(even, roll(hl, -1, 0), hr)
                    mine, code = cur[step, v, s], moves[step, s]
                    swapped = jnp.where(even, roll(mine, -1, 0), roll(mine, 1, 0))
                    from_halo = jnp.where(even, code, 8 - code) >= 6
                    mine = jnp.where(
                        (code >= 3) & (code < 6), mine, jnp.where(from_halo, outer, swapped)
                    )
                    dy = cy_ref[step, s]
                    fwd, bwd = roll(mine, LEVELS, 1), roll(mine, -LEVELS, 1)
                    fwd_in = jnp.where(row < 2, roll(low, -LEVELS * g, 1), roll(fwd, 2, 0))
                    bwd_in = jnp.where(row >= ROWS - 2, roll(high, -LEVELS * (g + 1), 1), roll(bwd, -2, 0))
                    fwd = jnp.where(group == 0, fwd_in, fwd)
                    bwd = jnp.where(group == groups - 1, bwd_in, bwd)
                    moved[v, s] = jnp.where(dy == 0, mine, jnp.where(dy > 0, fwd, bwd))
        if step == 0:
            wait(loads[2:])

        def pair_body(i, _):
            found = []
            for k in range(2):
                index = order[step, 2 * i + k]
                bits = [(index & (1 << b)) != 0 for b in range((slots - 1).bit_length())]
                for v in range(2):
                    found.append(tree([moved[v, s] for s in range(slots)], bits))
            na, ma, nb, mb = found
            na, nb, ma, mb = collide(na, nb, ma, mb, tries[step, i])
            paired[0, 2 * i] = na
            paired[0, 2 * i + 1] = nb
            paired[1, 2 * i] = ma
            paired[1, 2 * i + 1] = mb
            return 0

        lax.fori_loop(0, slots // 2, pair_body, 0)

        def slot_body(q, sums):
            base = q * width
            counts = [jnp.zeros((ROWS, LANES), jnp.float32)] * width
            masses = [jnp.zeros((ROWS, LANES), jnp.float32)] * width
            for p in range(slots):
                index = order[step, p] - base
                pn, pm = paired[0, p], paired[1, p]
                for k in range(width):
                    hit = index == k
                    counts[k] = jnp.where(hit, pn, counts[k])
                    masses[k] = jnp.where(hit, pm, masses[k])
            if step + 1 < steps:
                pack_sides(step + 1, q, 0, counts)
                pack_sides(step + 1, q, 1, masses)
            count, liquid = sums
            target = cur.at[step + 1] if step + 1 < steps else out_ref
            for k in range(width):
                target[0, base + k] = counts[k]
                target[1, base + k] = masses[k]
                count = count + counts[k]
                liquid = liquid + counts[k] * masses[k]
            if step + 1 < steps:
                store_rim(step + 1, q, 0, counts)
                store_rim(step + 1, q, 1, masses)
                pl.when(q == 0)(lambda: start(x_copies(step + 1, 0)))
            return count, liquid

        zero = jnp.zeros((ROWS, LANES), jnp.float32)
        sums = lax.fori_loop(0, CHUNKS, slot_body, (zero, zero))
        if step + 1 < steps:
            start(rim_copies(step + 1))
            for q in range(1, CHUNKS):
                start(x_copies(step + 1, q))
        for total in sums:
            shift = ROWS // 2
            while shift:
                total = total + roll(total, shift, 0)
                shift //= 2
            shift = LANES // 2
            while shift >= LEVELS:
                total = total + roll(total, shift, 1)
                shift //= 2
            row_totals.append(total)

    total = row_totals[0]
    for i in range(1, len(row_totals)):
        total = jnp.where(group == i, row_totals[i], total)
    total = total[0:1]
    for k, (size, me, device) in enumerate(stages):
        part, got, ss, rs = sums_refs[4 * k : 4 * k + 4]
        part[...] = total
        got[me] = total
        sends = [
            remote(part, got.at[me], ss.at[d - 1], rs.at[d - 1], device(lax.rem(me + d, size)))
            for d in range(1, size)
        ]
        start(sends)
        wait(sends)
        terms = [got[i] for i in range(size)]
        while len(terms) > 1:
            terms = [sum(terms[i + 1 : i + 2], terms[i]) for i in range(0, len(terms), 2)]
        total = terms[0]
    total = jnp.broadcast_to(total * scale, (ROWS, LANES))
    for i in range(steps):
        for v in range(2):
            mom_ref[i, v : v + 1, :] = roll(total, -LEVELS * (2 * i + v), 1)[0:1, :LEVELS]


def sum_stages(nx, ny, gx, gy):
    if nx * ny <= 64:
        return [(nx * ny, gx * ny + gy, lambda p: (p // ny, lax.rem(p, ny)))]
    return [(ny, gy, lambda p: (gx, p)), (nx, gx, lambda p: (p, gy))]


def solution(mesh):
    nx, ny = mesh.shape["gx"], mesh.shape["gy"]

    def body(droplets, moves, pairing, collisions):
        two, slots, cols, flat = droplets.shape
        steps, tiles = moves.shape[0], flat // LANES
        assert cols * tiles == ROWS and cols == 2

        def view(a):
            lead = a.shape[:2]
            return a.reshape(*lead, cols, tiles, LANES).swapaxes(2, 3).reshape(*lead, ROWS, LANES)

        f32, i32 = jnp.float32, jnp.int32
        tile = (ROWS, LANES)
        per = slots // 2 // CHUNKS
        dma = pltpu.SemaphoreType.DMA
        halo = pltpu.VMEM((steps, CHUNKS, 2, per, *tile), f32)
        edge = pltpu.VMEM((steps, 2, 2, *tile), f32)
        rim = pltpu.VMEM((steps, 2, *tile), f32)
        sums = []
        for size, _, _ in sum_stages(nx, ny, 0, 0):
            sums += [pltpu.VMEM((1, LANES), f32), pltpu.VMEM((size, 1, LANES), f32), dma((size - 1,)), dma((size - 1,))]
        code = pltpu.VMEM((steps, *tile), i32)
        scale = 1.0 / (cols * nx * (flat // LEVELS) * ny * count_unit)
        any_space = pl.BlockSpec(memory_space=pl.ANY)
        out, moments = pl.pallas_call(
            functools.partial(kernel, nx, ny, slots, steps, scale),
            out_shape=(
                pltpu.VMEM((two, slots, *tile), f32),
                jax.ShapeDtypeStruct((steps, 2, LEVELS), f32),
            ),
            in_specs=[any_space] * 4,
            out_specs=(pl.BlockSpec(memory_space=pltpu.VMEM), pl.BlockSpec(memory_space=pltpu.VMEM)),
            scratch_shapes=[
                pltpu.VMEM((steps, two, slots, *tile), f32),
                pltpu.VMEM((steps, slots, *tile), i32),
                pltpu.VMEM((steps, slots, *tile), i32),
                pltpu.VMEM((steps, slots // 2, *tile), i32),
                pltpu.VMEM((two, slots, *tile), f32),
                pltpu.VMEM((two, slots, *tile), f32),
                pltpu.VMEM((steps, slots, *tile), i32),
                halo, halo, halo, halo,
                code, code, code,
                edge, rim, rim, code, edge, edge, edge,
                dma((4,)),
                dma((steps, 2, CHUNKS)), dma((steps, CHUNKS)), dma((steps, CHUNKS)),
                dma((2,)), dma, dma,
                dma((steps, 2)), dma((steps,)), dma((steps,)),
                dma((steps, 2)), dma((steps,)), dma((steps,)),
                *sums,
            ],
            compiler_params=pltpu.CompilerParams(collective_id=0, has_side_effects=True),
        )(view(droplets), view(moves), view(pairing), view(collisions))
        out = out.reshape(two, slots, tiles, cols, LANES).swapaxes(2, 3).reshape(droplets.shape)
        return out, moments

    placed = P(None, None, "gx", "gy")
    return jax.shard_map(
        body, mesh=mesh, in_specs=(placed,) * 4, out_specs=(placed, P()), check_vma=False
    )
```
